32 devices in a mesh: fsdp: 16 (over z, y, core), tp: 2 (over x).
Axes of the slice: x: 2, y: 2, z: 4, core: 2. Of those that a mesh axis runs over, the one named last changes fastest.
Arguments:
- tokens: bfloat16 [6144, 5632], P('fsdp', 'tp'), may hold values from -6 to 6
- gain: float32 [5632], replicated, may hold values from 0.1 to 1.9
- query_projection_weight: bfloat16 [5632, 6144], P('fsdp', 'tp'), may hold values from -0.078125 to 0.078125
- key_projection_weight: bfloat16 [5632, 1024], P('fsdp', 'tp'), may hold values from -0.078125 to 0.078125
- value_projection_weight: bfloat16 [5632, 1024], P('fsdp', 'tp'), may hold values from -0.078125 to 0.078125
- adapter_down_factors: bfloat16 [3, 16, 5632], replicated, may hold values from -0.078125 to 0.078125
- query_adapter_up: bfloat16 [16, 6144], P(None, 'tp'), may hold values from -0.078125 to 0.078125
- key_adapter_up: bfloat16 [16, 1024], P(None, 'tp'), may hold values from -0.1875 to 0.1875
- value_adapter_up: bfloat16 [16, 1024], P(None, 'tp'), may hold values from -0.1875 to 0.1875
- query_cotangent: bfloat16 [6144, 6144], P('fsdp', 'tp'), may hold values from -6 to 6
- key_cotangent: bfloat16 [6144, 1024], P('fsdp', 'tp'), may hold values from -6 to 6
- value_cotangent: bfloat16 [6144, 1024], P('fsdp', 'tp'), may hold values from -6 to 6
Outputs:
- grad_tokens: bfloat16 [6144, 5632], P('fsdp', 'tp')
- grad_down: float32 [3, 16, 5632], P(None, None, 'tp')
- grad_up_query: float32 [16, 6144], P(None, 'tp')
- grad_up_key: float32 [16, 1024], P(None, 'tp')
- grad_up_value: float32 [16, 1024], P(None, 'tp')
The draws below stay inside these ranges and needn't reach their ends.
All inputs are finite; a program needn't handle non-finite values.
Results may differ from the reference program's by a relative error of at most 0.0096.
Values may be sent and summed in bfloat16 or wider, within the bound.
A program may use at most 128 MiB of HBM per device.

```python
import math
import jax
import jax.numpy as jnp
from jax import lax

MODEL_WIDTH = 5632
ADAPTER_RANK = 16
QUERY_WIDTH = 6144
KEY_VALUE_WIDTH = 1024
TOKEN_TOTAL = 6144


def steps_of(stream_key, dims, pieces, low, largest):
    factor_of = 1.0
    for dim, blocks in pieces:
        draws = jax.random.uniform(jax.random.fold_in(jax.random.fold_in(stream_key, 6), dim), (blocks,), jnp.float32, low / len(pieces), largest / len(pieces))
        factor_of = factor_of * jnp.repeat(jnp.exp(draws), dims[dim] // blocks).reshape((-1,) + (1,) * (len(dims) - 1 - dim))
    return factor_of


def scatter_about(key, extent, scale, most, split=(), kind=jnp.bfloat16):
    level = steps_of(key, extent, split, -0.22, 0.18) if split else 1.0
    drawn = jax.random.normal(key, extent, jnp.float32) * scale * level
    return jnp.minimum(jnp.maximum(drawn, -most), most).astype(kind)


def setup_inputs(seed: int = 0) -> dict:
    splits = jax.random.split(jax.random.key(seed), 13)
    return {
        "tokens": scatter_about(splits[0], (TOKEN_TOTAL, MODEL_WIDTH), 1.0, 6.0, ((0, 16), (1, 2))),
        "gain": jnp.clip(1.0 + 0.18 * jax.random.normal(splits[1], (MODEL_WIDTH,), jnp.float32), 0.1, 1.9),
        "query_projection_weight": scatter_about(splits[2], (MODEL_WIDTH, QUERY_WIDTH), MODEL_WIDTH ** -0.5, 0.078125, ((0, 16), (1, 2))),
        "key_projection_weight": scatter_about(splits[3], (MODEL_WIDTH, KEY_VALUE_WIDTH), MODEL_WIDTH ** -0.5, 0.078125, ((0, 16), (1, 2))),
        "value_projection_weight": scatter_about(splits[4], (MODEL_WIDTH, KEY_VALUE_WIDTH), MODEL_WIDTH ** -0.5, 0.078125, ((0, 16), (1, 2))),
        "adapter_down_factors": scatter_about(splits[5], (3, ADAPTER_RANK, MODEL_WIDTH), MODEL_WIDTH ** -0.5, 0.078125),
        "query_adapter_up": scatter_about(splits[6], (ADAPTER_RANK, QUERY_WIDTH), QUERY_WIDTH ** -0.5, 0.078125, ((1, 2),)),
        "key_adapter_up": scatter_about(splits[7], (ADAPTER_RANK, KEY_VALUE_WIDTH), KEY_VALUE_WIDTH ** -0.5, 0.1875, ((1, 2),)),
        "value_adapter_up": scatter_about(splits[8], (ADAPTER_RANK, KEY_VALUE_WIDTH), KEY_VALUE_WIDTH ** -0.5, 0.1875, ((1, 2),)),
        "query_cotangent": scatter_about(splits[9], (TOKEN_TOTAL, QUERY_WIDTH), 1.0, 6.0, ((0, 16), (1, 2))),
        "key_cotangent": scatter_about(splits[10], (TOKEN_TOTAL, KEY_VALUE_WIDTH), 1.0, 6.0, ((0, 16), (1, 2))),
        "value_cotangent": scatter_about(splits[11], (TOKEN_TOTAL, KEY_VALUE_WIDTH), 1.0, 6.0, ((0, 16), (1, 2))),
    }


norm_eps = 1e-05
adapter_scale = 2.0

def reference(tokens, gain, query_projection_weight, key_projection_weight, value_projection_weight, adapter_down_factors, query_adapter_up, key_adapter_up, value_adapter_up, query_cotangent, key_cotangent, value_cotangent):
    weights = (query_projection_weight, key_projection_weight, value_projection_weight)
    adapter_up_factors = (query_adapter_up, key_adapter_up, value_adapter_up)
    cotangent_list = (query_cotangent, key_cotangent, value_cotangent)
    token_width_matrix = tokens.astype(jnp.float32)
    inverse_root_mean = lax.rsqrt(lax.optimization_barrier(jnp.mean(token_width_matrix * token_width_matrix, axis=1, keepdims=True)) + norm_eps)
    unit_rows = token_width_matrix * inverse_root_mean
    scaled_input = unit_rows * gain[None, :]
    normed = scaled_input.astype(jnp.bfloat16)
    adapter_input = jnp.stack([jnp.dot(scaled_input, adapter_down_factors[slice_member].astype(jnp.float32).T, precision=lax.Precision.HIGHEST) for slice_member in range(3)])
    adapter_output = jnp.stack([jnp.dot(cotangent_list[slice_member], adapter_up_factors[slice_member].T, preferred_element_type=jnp.float32) for slice_member in range(3)])
    input_lowrank = adapter_input.astype(jnp.bfloat16)
    output_lowrank = adapter_output.astype(jnp.bfloat16)
    gradient_scale = adapter_scale / math.sqrt(TOKEN_TOTAL)
    backward_result = jnp.zeros(tokens.shape, jnp.float32)
    for slice_member in range(3):
        backward_result = backward_result + jnp.dot(cotangent_list[slice_member], weights[slice_member].T, preferred_element_type=jnp.float32)
    for slice_member in range(3):
        backward_result = backward_result + adapter_scale * jnp.dot(output_lowrank[slice_member], adapter_down_factors[slice_member], preferred_element_type=jnp.float32)
    gained = gain[None, :] * backward_result
    inner = lax.optimization_barrier(jnp.mean(gained * unit_rows, axis=1, keepdims=True))
    grad_tokens = (inverse_root_mean * (gained - unit_rows * inner)).astype(jnp.bfloat16)
    grad_down = jnp.stack([gradient_scale * jnp.dot(output_lowrank[slice_member].T, normed, preferred_element_type=jnp.float32) for slice_member in range(3)])
    grad_ups = [gradient_scale * jnp.dot(input_lowrank[slice_member].T, cotangent_list[slice_member], preferred_element_type=jnp.float32) for slice_member in range(3)]
    return (grad_tokens, grad_down, grad_ups[0], grad_ups[1], grad_ups[2])
```

```python
import math

import jax
import jax.numpy as jnp
from jax import lax
from jax.sharding import PartitionSpec as P


norm_eps = 1e-05
adapter_scale = 2.0
late_shares = (0.5, 0.82)


def transposed_product(left, right):
    return lax.dot_general(
        left, right, (((1,), (1,)), ((), ())), preferred_element_type=jnp.float32
    )


def plain_back(weights, cotangents, full_width):
    total = jnp.zeros((cotangents[0].shape[0], full_width), jnp.float32)
    for weight, cotangent in zip(weights, cotangents):
        whole = lax.all_gather(weight, "fsdp", axis=0, tiled=True)
        total = total + transposed_product(cotangent, whole)
    return lax.psum_scatter(total, "tp", scatter_dimension=1, tiled=True)


def chunk_bounds(rows):
    cuts = [0] + [16 * int(rows * share / 16) for share in late_shares] + [rows]
    return [(low, high) for low, high in zip(cuts[:-1], cuts[1:])]


def grid_back(weights, cotangents, small_work):
    size = lax.axis_size("fsdp")
    top = size // 2
    place = lax.axis_index("fsdp")
    half = lax.axis_index("tp")

    def swap(value, bit):
        return lax.ppermute(value, "fsdp", [(i, i ^ bit) for i in range(size)])

    def cross(value, early):
        pairs = []
        for i in range(size):
            for t in range(2):
                if ((i // top) == t) != early:
                    pairs.append((2 * i + t, 2 * i + 1 - t))
        return lax.ppermute(value, ("fsdp", "tp"), pairs)

    cot = jnp.concatenate(cotangents, axis=1)
    weight = jnp.concatenate(weights, axis=1)
    rows = weight.shape[0]
    tokens_here = cot.shape[0]
    bounds = chunk_bounds(rows)

    cot_z = swap(cot, 4)
    far = [swap(weight[low:high], top) for low, high in bounds]
    weight_y = swap(weight, 2)
    cot_c = swap(cot, 1)
    mine = (place // top) == half

    def product(piece, cots):
        return transposed_product(piece, cots).astype(jnp.bfloat16)

    near_cot = jnp.concatenate([cot, cot_c], axis=0)
    early_weight = jnp.concatenate([weight, weight_y], axis=0)
    early = [product(early_weight, near_cot)]
    _, early[0], far[0] = lax.optimization_barrier((small_work, early[0], far[0]))
    early_got = [cross(early[0], True)]
    far_y = [swap(far[0], 2)]
    cot_zc = swap(cot_z, 1)
    far_cot = jnp.concatenate([cot_z, cot_zc], axis=0)
    early.append(product(early_weight, far_cot))
    early[1], far[1] = lax.optimization_barrier((early[1], far[1]))
    early_got.append(cross(early[1], True))
    far_y += [swap(far[index], 2) for index in range(1, len(bounds))]
    all_cot = jnp.concatenate([near_cot, far_cot], axis=0)
    late = [product(jnp.concatenate(pair, axis=0), all_cot) for pair in zip(far, far_y)]
    late_got = [cross(part, False) for part in late]

    def add(a, b):
        return a.astype(jnp.float32) + b.astype(jnp.float32)

    blocks = [[None] * len(bounds) for _ in range(8)]
    for index, (low, high) in enumerate(bounds):
        depth = high - low
        l = add(late[index], late_got[index]).reshape(2, depth, -1)
        sums = []
        for side in range(2):
            e = add(early[side], early_got[side]).reshape(2, rows, -1)[:, low:high]
            l_side = l[..., 2 * tokens_here * side : 2 * tokens_here * (side + 1)]
            sums.append(jnp.where(mine, e, l_side).astype(jnp.bfloat16))
        near, far_sum = sums
        got = swap(far_sum, 4)
        send = jnp.concatenate([near[..., tokens_here:], got[..., tokens_here:]], axis=2)
        other = swap(send, 1)
        four = (
            near[..., :tokens_here],
            other[..., :tokens_here],
            got[..., :tokens_here],
            other[..., tokens_here:],
        )
        for relative, block in zip((0, 1, 4, 5), four):
            for member in range(2):
                blocks[relative ^ (2 * member)][index] = block[member]
    result = jnp.stack([jnp.concatenate(parts, axis=0) for parts in blocks])
    base = place % top
    for bit in (1, 2, 4):
        pair = result.reshape(8 // (2 * bit), 2, bit, rows, tokens_here)
        result = jnp.where((base // bit) % 2 == 1, pair[:, ::-1], pair)
    result = result.reshape(top * rows, tokens_here)
    return result.T.astype(jnp.float32)


def shards(
    tokens,
    gain,
    query_projection_weight,
    key_projection_weight,
    value_projection_weight,
    adapter_down_factors,
    query_adapter_up,
    key_adapter_up,
    value_adapter_up,
    query_cotangent,
    key_cotangent,
    value_cotangent,
):
    return device_work(
        tokens,
        gain,
        (query_projection_weight, key_projection_weight, value_projection_weight),
        adapter_down_factors,
        (query_adapter_up, key_adapter_up, value_adapter_up),
        (query_cotangent, key_cotangent, value_cotangent),
    )


def device_work(tokens, gain, weights, adapter_down_factors, ups, cots):
    fsdp_size = lax.axis_size("fsdp")
    tp_size = lax.axis_size("tp")
    tp_index = lax.axis_index("tp")
    row_count, owned = tokens.shape
    full_width = gain.shape[0]
    rank = adapter_down_factors.shape[1]

    def tp_sum(value):
        if tp_size != 2:
            return lax.psum(value, "tp")
        return value + lax.ppermute(value, "tp", [(0, 1), (1, 0)])

    wide = tokens.astype(jnp.float32)
    gain_own = lax.dynamic_slice_in_dim(gain, tp_index * owned, owned, 0)
    down = lax.dynamic_slice_in_dim(adapter_down_factors, tp_index * owned, owned, 2)
    down = down.reshape(3 * rank, owned)
    low_in = lax.dot_general(
        wide * gain_own[None, :],
        down.astype(jnp.float32),
        (((1,), (1,)), ((), ())),
        precision=lax.Precision.HIGHEST,
    )
    low_out = jnp.concatenate([transposed_product(c, u) for c, u in zip(cots, ups)], axis=1)
    squares = jnp.sum(wide * wide, axis=1, keepdims=True)
    small = tp_sum(jnp.concatenate([squares, low_in, low_out], axis=1))
    inverse = lax.rsqrt(small[:, :1] / full_width + norm_eps)
    in_low = (small[:, 1 : 1 + 3 * rank] * inverse).astype(jnp.bfloat16)
    out_low = small[:, 1 + 3 * rank :].astype(jnp.bfloat16)
    unit_rows = wide * inverse
    normed = (unit_rows * gain_own[None, :]).astype(jnp.bfloat16)
    scale = adapter_scale / math.sqrt(row_count * fsdp_size)

    def token_product(left, right):
        return scale * lax.dot_general(
            left, right, (((0,), (0,)), ((), ())), preferred_element_type=jnp.float32
        )

    down_local = token_product(out_low, normed)
    up_local = [
        token_product(in_low[:, rank * m : rank * (m + 1)], cots[m]) for m in range(3)
    ]
    small_work = tuple(down_local[rank * m : rank * (m + 1)] for m in range(3)) + tuple(up_local)
    if tp_size == 2 and fsdp_size == 16:
        back = grid_back(weights, cots, small_work)
    else:
        back = plain_back(weights, cots, full_width)
    grads = lax.psum(jnp.concatenate(small_work, axis=1), "fsdp")
    grad_down = jnp.stack([grads[:, owned * m : owned * (m + 1)] for m in range(3)])
    ends = [3 * owned]
    for cot in cots:
        ends.append(ends[-1] + cot.shape[1])
    up_q, up_k, up_v = [grads[:, low:high] for low, high in zip(ends[:-1], ends[1:])]

    back = back + adapter_scale * jnp.dot(out_low, down, preferred_element_type=jnp.float32)
    gained = gain_own[None, :] * back
    inner = tp_sum(jnp.sum(gained * unit_rows, axis=1, keepdims=True)) / full_width
    grad_tokens = (inverse * (gained - unit_rows * inner)).astype(jnp.bfloat16)
    return (grad_tokens, grad_down, up_q, up_k, up_v)


def solution(mesh):
    in_specs = (
        P("fsdp", "tp"),
        P(),
        P("fsdp", "tp"),
        P("fsdp", "tp"),
        P("fsdp", "tp"),
        P(),
        P(None, "tp"),
        P(None, "tp"),
        P(None, "tp"),
        P("fsdp", "tp"),
        P("fsdp", "tp"),
        P("fsdp", "tp"),
    )
    out_specs = (P("fsdp", "tp"), P(None, None, "tp"), P(None, "tp"), P(None, "tp"), P(None, "tp"))
    return jax.shard_map(shards, mesh=mesh, in_specs=in_specs, out_specs=out_specs, check_vma=False)
```
